32 devices in a mesh: row: 4 (over x, core), col: 8 (over z, y).
Axes of the slice: x: 2, y: 2, z: 4, core: 2. Of those that a mesh axis runs over, the one named last changes fastest.
Arguments:
- x_rows: float32 [16, 16384], P(None, ('row', 'col')), may hold values from -6 to 6
- alpha_rows: float32 [16384], P(('row', 'col')), may hold values from -0.5 to 1.5
- x_cols: float32 [16, 8192], P(None, ('col', 'row')), may hold values from -6 to 6
- alpha_cols: float32 [8192], P(('col', 'row')), may hold values from -0.0073242188 to 0.021972656
- lengthscale: float32 [16], replicated, may hold values from 1.2 to 2.5
Outputs:
- row_terms: float32 [16, 16384], P(None, ('row', 'col'))
- kernel_alpha: float32 [16384], P(('row', 'col'))
- grad: float32 [16], replicated
The draws below stay inside these ranges and needn't reach their ends.
All inputs are finite; a program needn't handle non-finite values.
Results may differ from the reference program's by a relative error of at most 0.00021.
Values sent between devices are 32-bit elements; how exact they have to be, the bound alone decides.
A program may use at most 64 MiB of HBM per device.

```python
import math
import jax
import jax.numpy as jnp
from jax import lax

DIMS = 16
ROWS = 16384
NPTS = 8192


def block_levels(rng, shape, split, low, high):
    gain = 1.0
    for position, parts in split:
        draws = jax.random.uniform(jax.random.fold_in(jax.random.fold_in(rng, 6), position), (parts,), jnp.float32, low / len(split), high / len(split))
        gain = gain * jnp.repeat(jnp.exp(draws), shape[position] // parts).reshape((-1,) + (1,) * (len(shape) - 1 - position))
    return gain


def bell_draw(stream_key, extent, spread, most, shards=(), kind=jnp.bfloat16):
    entries = jax.random.normal(stream_key, extent, jnp.float32) * spread
    if len(shards) > 0:
        entries = block_levels(stream_key, extent, shards, -0.22, 0.18) * entries
    return jnp.clip(entries, min=-most, max=most).astype(kind)


def setup_inputs(seed: int = 0) -> dict:
    seeds = jax.random.split(jax.random.key(seed), 6)
    return {
        "x_rows": bell_draw(seeds[0], (DIMS, ROWS), 1.0, 6.0, ((1, 32),), jnp.float32),
        "alpha_rows": jnp.clip(-0.5 + 2.0 * jax.random.uniform(seeds[1], (ROWS,), jnp.float32) ** block_levels(seeds[1], (ROWS,), ((0, 32),), -0.2, 0.2), -0.5, 1.5),
        "x_cols": bell_draw(seeds[2], (DIMS, NPTS), 1.0, 6.0, ((1, 32),), jnp.float32),
        "alpha_cols": jnp.clip(-0.0073242188 + 0.029296875 * jax.random.uniform(seeds[3], (NPTS,), jnp.float32) ** block_levels(seeds[3], (NPTS,), ((0, 32),), -0.2, 0.2), -0.0073242188, 0.021972656),
        "lengthscale": jnp.clip(jnp.exp(jax.random.uniform(seeds[4], (DIMS,), jnp.float32, math.log(1.2), math.log(2.5))), 1.2, 2.5),
    }


def fold_terms(partials, row_scaled, row_alpha):
    dims = row_scaled.shape[0]
    weight_sum = partials[0]
    first_moment = partials[1:1 + dims]
    second_moment = partials[1 + dims:]
    terms = 0.5 * row_alpha[None, :] * (row_scaled * row_scaled * weight_sum[None, :] - 2.0 * row_scaled * first_moment + second_moment)
    return terms, weight_sum


def reference(x_rows, alpha_rows, x_cols, alpha_cols, lengthscale):
    inverse_scale = 1.0 / lengthscale
    row_scaled = x_rows * inverse_scale[:, None]
    col_scaled = x_cols * inverse_scale[:, None]
    col_norms = jnp.sum(col_scaled * col_scaled, 0)
    values = jnp.concatenate([alpha_cols[None, :], alpha_cols[None, :] * col_scaled, alpha_cols[None, :] * col_scaled * col_scaled], 0)
    block_rows = min(512, ROWS)
    block_count = ROWS // block_rows
    blocks = jnp.transpose(row_scaled.reshape(DIMS, block_count, block_rows), (1, 0, 2))

    def one_block(row_block):
        row_norms = jnp.sum(row_block * row_block, 0)
        cross = lax.dot_general(row_block, col_scaled, (((0,), (0,)), ((), ())), precision=lax.Precision.HIGHEST, preferred_element_type=jnp.float32)
        kernel = jnp.exp(-0.5 * (row_norms[:, None] + col_norms[None, :] - 2.0 * cross))
        return lax.dot_general(values, kernel, (((1,), (1,)), ((), ())), precision=lax.Precision.HIGHEST, preferred_element_type=jnp.float32)

    pieces = lax.map(one_block, blocks)
    partials = jnp.transpose(pieces, (1, 0, 2)).reshape(2 * DIMS + 1, ROWS)
    terms, weight_sum = fold_terms(partials, row_scaled, alpha_rows)
    grad = jnp.sum(terms, 1) / ROWS
    return terms, weight_sum, grad
```

```python
import functools

import jax
import jax.numpy as jnp
from jax import lax
from jax.experimental import pallas as pl
from jax.experimental.pallas import tpu as pltpu
from jax.sharding import PartitionSpec as P

LOG2E = 1.4426950408889634
CORES = 2
MESH = pl.DeviceIdType.MESH
F32 = jnp.float32
BF16 = jnp.bfloat16


def split3(value):
    high = value.astype(BF16)
    rest = value - high.astype(F32)
    mid = rest.astype(BF16)
    low = (rest - mid.astype(F32)).astype(BF16)
    return high, mid, low


def stack_rows(count, rows):
    index = lax.broadcasted_iota(jnp.int32, (16, count), 0)
    out = jnp.zeros((16, count), F32)
    for place, row in enumerate(rows):
        row = row.astype(F32) if hasattr(row, "astype") else row
        out = jnp.where(index == place, row, out)
    return out.astype(BF16)


def kernel(
    row_size,
    col_size,
    xr_ref,
    ar_ref,
    xc_ref,
    ac_ref,
    ls_ref,
    terms_ref,
    sums_ref,
    grad_ref,
    xg,
    ag,
    acc,
    row_aug,
    part,
    parts,
    send_x,
    recv_x,
    send_a,
    recv_a,
    send_f,
    recv_f,
    send_b,
    recv_b,
    send_g,
    recv_g,
):
    dims, row_count = xr_ref.shape
    col_count = xc_ref.shape[1]
    n_x = row_size // CORES
    n = n_x * col_size
    n_all = row_size * col_size
    my_row = lax.axis_index("row")
    my_col = lax.axis_index("col")
    partner = (my_row + 1 - 2 * (my_row % CORES), my_col)

    def plane_peer(step):
        d_x = step % n_x
        d_col = step // n_x
        return ((my_row + CORES * d_x) % row_size, (my_col + d_col) % col_size)

    def any_peer(step):
        d_row = step % row_size
        d_col = step // row_size
        return ((my_row + d_row) % row_size, (my_col + d_col) % col_size)

    barrier = pltpu.get_barrier_semaphore()

    @pl.loop(1, n_all)
    def _(step):
        pl.semaphore_signal(barrier, inc=1, device_id=any_peer(step), device_id_type=MESH)

    def x_copy(step):
        return pltpu.make_async_remote_copy(
            xc_ref, xg.at[step], send_x.at[step], recv_x.at[step], plane_peer(step), MESH
        )

    def a_copy(step):
        return pltpu.make_async_remote_copy(
            ac_ref, ag.at[step], send_a.at[step], recv_a.at[step], plane_peer(step), MESH
        )

    def x_forward(step, src):
        return pltpu.make_async_remote_copy(
            src, xg.at[n + step], send_f.at[step], recv_f.at[step], partner, MESH
        )

    def a_forward(step, src):
        return pltpu.make_async_remote_copy(
            src, ag.at[n + step], send_b.at[step], recv_b.at[step], partner, MESH
        )

    def g_copy(step):
        return pltpu.make_async_remote_copy(
            part.at[pl.ds(0, 1)],
            parts.at[step],
            send_g.at[step],
            recv_g.at[step],
            any_peer(step),
            MESH,
        )

    eye = lax.broadcasted_iota(jnp.int32, (dims, dims), 0) == lax.broadcasted_iota(
        jnp.int32, (dims, dims), 1
    )
    scale = jnp.sum(jnp.where(eye, jnp.broadcast_to(ls_ref[...], (dims, dims)), 0.0), 1, keepdims=True)
    inverse = 1.0 / scale
    row_scaled = xr_ref[...] * inverse
    row_norm = (-0.5 * LOG2E) * jnp.sum(row_scaled * row_scaled, 0, keepdims=True)
    rh, rm, rl = split3(row_scaled * LOG2E)
    row_aug[...] = jnp.concatenate(
        [rh, rh, rh, rm, rm, rl, stack_rows(row_count, (1.0, 1.0, 1.0) + split3(row_norm))], 0
    )

    def operands(x, alpha):
        scaled = x * inverse
        norm = (-0.5 * LOG2E) * jnp.sum(scaled * scaled, 0, keepdims=True)
        ch, cm, cl = split3(scaled)
        col_aug = jnp.concatenate(
            [ch, cm, cl, ch, cm, ch, stack_rows(col_count, split3(norm) + (1.0, 1.0, 1.0))], 0
        )
        first = alpha * scaled
        fh, fm, fl = split3(first)
        sh, sm, sl = split3(first * scaled)
        group = stack_rows(col_count, split3(alpha))
        zero = jnp.zeros_like(fl)
        left_high = jnp.concatenate([fh, sh, fm, sm, fl, sl, group], 0)
        left_mid = jnp.concatenate([fh, sh, fm, sm, zero, zero, group], 0)
        exponent = lax.dot_general(
            col_aug, row_aug[...], (((0,), (0,)), ((), ())), preferred_element_type=F32
        )
        value = jnp.exp2(exponent)
        high = value.astype(BF16)
        mid = (value - high.astype(F32)).astype(BF16)
        return [left_high, left_mid], [high, mid]

    def contribute(chunks):
        left, right = [], []
        for x, alpha in chunks:
            more_left, more_right = operands(x, alpha)
            left += more_left
            right += more_right
        return jnp.dot(
            jnp.concatenate(left, 1), jnp.concatenate(right, 0), preferred_element_type=F32
        )

    acc[...] = contribute([(xc_ref[...], ac_ref[...])])

    pl.semaphore_wait(barrier, n_all - 1)
    x_forward(0, xc_ref).start()
    a_forward(0, ac_ref).start()

    @pl.loop(1, n)
    def _(step):
        x_copy(step).start()
        a_copy(step).start()

    @pl.loop(1, n)
    def _(step):
        x_copy(step).wait_recv()
        a_copy(step).wait_recv()
        x_forward(step, xg.at[step]).start()
        a_forward(step, ag.at[step]).start()
        x_forward(step - 1, xg.at[step]).wait_recv()
        a_forward(step - 1, ag.at[step]).wait_recv()
        acc[...] += contribute(
            [(xg[step], ag[step]), (xg[n + step - 1], ag[n + step - 1])]
        )

    x_forward(n - 1, xc_ref).wait_recv()
    a_forward(n - 1, ac_ref).wait_recv()
    total = acc[...] + contribute([(xg[2 * n - 1], ag[2 * n - 1])])
    first = total[0:16] + total[32:48] + total[64:80]
    second = total[16:32] + total[48:64] + total[80:96]
    weight = total[96:97] + total[97:98] + total[98:99]
    terms = (0.5 * ar_ref[...]) * (
        row_scaled * row_scaled * weight - 2.0 * row_scaled * first + second
    )
    folded = terms[:, 0:128]
    for at in range(128, row_count, 128):
        folded = folded + terms[:, at : at + 128]
    gathered = lax.dot_general(
        jnp.ones((8, 128), F32),
        folded,
        (((1,), (1,)), ((), ())),
        precision=lax.Precision.HIGHEST,
        preferred_element_type=F32,
    )
    part[...] = jnp.zeros_like(part)
    part[:, 0:dims] = gathered
    terms_ref[...] = terms
    sums_ref[...] = weight

    @pl.loop(1, n)
    def _(step):
        x_copy(step).wait_send()
        a_copy(step).wait_send()

    @pl.loop(0, n)
    def _(step):
        x_forward(step, xc_ref).wait_send()
        a_forward(step, ac_ref).wait_send()

    @pl.loop(1, n_all)
    def _(step):
        g_copy(step).start()

    parts[0] = part[0:1]

    @pl.loop(1, n_all)
    def _(step):
        g_copy(step).wait()

    grad_ref[...] = (jnp.sum(parts[...], 0) / (row_count * n_all))[:, 0:dims]


def on_device(row_size, col_size, x_rows, alpha_rows, x_cols, alpha_cols, lengthscale):
    dims, row_count = x_rows.shape
    col_count = x_cols.shape[1]
    n = row_size // CORES * col_size
    n_all = row_size * col_size
    vmem = pl.BlockSpec(memory_space=pltpu.VMEM)
    dma = pltpu.SemaphoreType.DMA
    terms, sums, grad = pl.pallas_call(
        functools.partial(kernel, row_size, col_size),
        out_shape=(
            jax.ShapeDtypeStruct((dims, row_count), F32),
            jax.ShapeDtypeStruct((1, row_count), F32),
            jax.ShapeDtypeStruct((1, dims), F32),
        ),
        in_specs=[vmem] * 5,
        out_specs=(vmem, vmem, vmem),
        scratch_shapes=[
            pltpu.VMEM((2 * n, dims, col_count), F32),
            pltpu.VMEM((2 * n, 1, col_count), F32),
            pltpu.VMEM((112, row_count), F32),
            pltpu.VMEM((112, row_count), BF16),
            pltpu.VMEM((8, 128), F32),
            pltpu.VMEM((n_all, 1, 128), F32),
        ]
        + [dma((n,))] * 8
        + [dma((n_all,))] * 2,
        compiler_params=pltpu.CompilerParams(collective_id=0, has_side_effects=True),
    )(
        x_rows,
        alpha_rows.reshape(1, row_count),
        x_cols,
        alpha_cols.reshape(1, col_count),
        lengthscale.reshape(1, dims),
    )
    return terms, sums.reshape(row_count), grad.reshape(dims)


def solution(mesh):
    return jax.shard_map(
        functools.partial(on_device, mesh.shape["row"], mesh.shape["col"]),
        mesh=mesh,
        in_specs=(
            P(None, ("row", "col")),
            P(("row", "col")),
            P(None, ("col", "row")),
            P(("col", "row")),
            P(),
        ),
        out_specs=(P(None, ("row", "col")), P(("row", "col")), P()),
        check_vma=False,
    )
```

```python
import functools

import jax
import jax.numpy as jnp
from jax import lax
from jax.experimental import pallas as pl
from jax.experimental.pallas import tpu as pltpu
from jax.sharding import PartitionSpec as P

LOG2E = 1.4426950408889634
CORES = 2
MESH = pl.DeviceIdType.MESH
F32 = jnp.float32
BF16 = jnp.bfloat16


def split3(value):
    high = value.astype(BF16)
    rest = value - high.astype(F32)
    mid = rest.astype(BF16)
    low = (rest - mid.astype(F32)).astype(BF16)
    return high, mid, low


def stack_rows(count, rows):
    index = lax.broadcasted_iota(jnp.int32, (16, count), 0)
    out = jnp.zeros((16, count), F32)
    for place, row in enumerate(rows):
        row = row.astype(F32) if hasattr(row, "astype") else row
        out = jnp.where(index == place, row, out)
    return out.astype(BF16)


def kernel(
    row_size,
    col_size,
    xr_hbm,
    ar_hbm,
    xc_hbm,
    ac_hbm,
    ls_hbm,
    terms_hbm,
    sums_hbm,
    grad_hbm,
    xr_ref,
    ar_ref,
    ls_ref,
    terms_ref,
    sums_ref,
    grad_ref,
    chunks,
    acc,
    row_aug,
    part,
    parts,
    local,
    send_c,
    recv_c,
    send_f,
    recv_f,
    send_g,
    recv_g,
):
    dims, row_count = xr_ref.shape
    col_count = chunks.shape[2]
    n_x = row_size // CORES
    n_y = n_x if col_size % n_x == 0 else 1
    n_z = col_size // n_y
    n_plane = n_x * n_y
    n = n_x * col_size
    n_all = row_size * col_size
    my_row = lax.axis_index("row")
    my_col = lax.axis_index("col")
    my_z = my_col // n_y
    my_y = my_col % n_y
    partner = (my_row + 1 - 2 * (my_row % CORES), my_col)

    def line_peer(j):
        return (my_row, (my_z + j) % n_z * n_y + my_y)

    def plane_peer(m):
        return (
            (my_row + CORES * (m % n_x)) % row_size,
            my_z * n_y + (my_y + m // n_x) % n_y,
        )

    def any_peer(step):
        d_row = step % row_size
        d_col = step // row_size
        return ((my_row + d_row) % row_size, (my_col + d_col) % col_size)

    def loads():
        return [
            pltpu.make_async_copy(xc_hbm, chunks.at[0, pl.ds(0, dims)], local.at[0]),
            pltpu.make_async_copy(ac_hbm, chunks.at[0, pl.ds(dims, 1)], local.at[1]),
            pltpu.make_async_copy(xr_hbm, xr_ref, local.at[2]),
            pltpu.make_async_copy(ar_hbm, ar_ref, local.at[3]),
            pltpu.make_async_copy(ls_hbm, ls_ref, local.at[4]),
        ]

    for copy in loads():
        copy.start()

    barrier = pltpu.get_barrier_semaphore()

    pl.semaphore_signal(barrier, inc=1, device_id=partner, device_id_type=MESH)

    @pl.loop(1, n_plane)
    def _(m):
        pl.semaphore_signal(barrier, inc=1, device_id=plane_peer(m), device_id_type=MESH)

    @pl.loop(1, n_z)
    def _(j):
        pl.semaphore_signal(barrier, inc=1, device_id=line_peer(j), device_id_type=MESH)

    def line_copy(j):
        return pltpu.make_async_remote_copy(
            chunks.at[0], chunks.at[j], send_c.at[j], recv_c.at[j], line_peer(j), MESH
        )

    def plane_copy(j, m):
        slot = m * n_z + j
        return pltpu.make_async_remote_copy(
            chunks.at[j], chunks.at[slot], send_c.at[slot], recv_c.at[slot], plane_peer(m), MESH
        )

    def forward(slot):
        return pltpu.make_async_remote_copy(
            chunks.at[slot], chunks.at[n + slot], send_f.at[slot], recv_f.at[slot], partner, MESH
        )

    def g_copy(step):
        return pltpu.make_async_remote_copy(
            part.at[pl.ds(0, 1)],
            parts.at[step],
            send_g.at[step],
            recv_g.at[step],
            any_peer(step),
            MESH,
        )

    for copy in loads():
        copy.wait()

    eye = lax.broadcasted_iota(jnp.int32, (dims, dims), 0) == lax.broadcasted_iota(
        jnp.int32, (dims, dims), 1
    )
    scale = jnp.sum(jnp.where(eye, jnp.broadcast_to(ls_ref[...], (dims, dims)), 0.0), 1, keepdims=True)
    inverse = 1.0 / scale
    row_scaled = xr_ref[...] * inverse
    row_norm = (-0.5 * LOG2E) * jnp.sum(row_scaled * row_scaled, 0, keepdims=True)
    rh, rm, rl = split3(row_scaled * LOG2E)
    row_aug[...] = jnp.concatenate(
        [rh, rh, rh, rm, rm, rl, stack_rows(row_count, (1.0, 1.0, 1.0) + split3(row_norm))], 0
    )

    def operands(x, alpha):
        scaled = x * inverse
        norm = (-0.5 * LOG2E) * jnp.sum(scaled * scaled, 0, keepdims=True)
        ch, cm, cl = split3(scaled)
        col_aug = jnp.concatenate(
            [ch, cm, cl, ch, cm, ch, stack_rows(col_count, split3(norm) + (1.0, 1.0, 1.0))], 0
        )
        first = alpha * scaled
        fh, fm, fl = split3(first)
        sh, sm, sl = split3(first * scaled)
        group = stack_rows(col_count, split3(alpha))
        zero = jnp.zeros_like(fl)
        left_high = jnp.concatenate([fh, sh, fm, sm, fl, sl, group], 0)
        left_mid = jnp.concatenate([fh, sh, fm, sm, zero, zero, group], 0)
        exponent = lax.dot_general(
            col_aug, row_aug[...], (((0,), (0,)), ((), ())), preferred_element_type=F32
        )
        value = jnp.exp2(exponent)
        high = value.astype(BF16)
        mid = (value - high.astype(F32)).astype(BF16)
        return [left_high, left_mid], [high, mid]

    def contribute(slots):
        left, right = [], []
        for slot in slots:
            more_left, more_right = operands(
                chunks[slot, 0:dims], chunks[slot, dims : dims + 1]
            )
            left += more_left
            right += more_right
        return jnp.dot(
            jnp.concatenate(left, 1), jnp.concatenate(right, 0), preferred_element_type=F32
        )

    acc[...] = contribute([0])

    pl.semaphore_wait(barrier, n_plane + n_z - 1)

    @pl.loop(1, n_z)
    def _(j):
        line_copy(j).start()

    @pl.loop(1, n_plane)
    def _(m):
        plane_copy(0, m).start()

    forward(0).start()
    forward(0).wait_recv()
    acc[...] += contribute([n])

    @pl.loop(1, n_z)
    def _(j):
        line_copy(j).wait_recv()

        @pl.loop(1, n_plane)
        def _(m):
            plane_copy(j, m).start()

        forward(j).start()
        acc[...] += contribute([j])

    lag = n_z - 1

    @pl.loop(n_z, n)
    def _(slot):
        line_copy(slot).wait_recv()
        forward(slot).start()
        forward(slot - lag).wait_recv()
        acc[...] += contribute([slot, n + slot - lag])

    @pl.loop(n - lag, n)
    def _(slot):
        forward(slot).wait_recv()
        acc[...] += contribute([n + slot])

    total = acc[...]
    first = total[0:16] + total[32:48] + total[64:80]
    second = total[16:32] + total[48:64] + total[80:96]
    weight = total[96:97] + total[97:98] + total[98:99]
    terms = (0.5 * ar_ref[...]) * (
        row_scaled * row_scaled * weight - 2.0 * row_scaled * first + second
    )
    folded = terms[:, 0:128]
    for at in range(128, row_count, 128):
        folded = folded + terms[:, at : at + 128]
    gathered = lax.dot_general(
        jnp.ones((8, 128), F32),
        folded,
        (((1,), (1,)), ((), ())),
        precision=lax.Precision.HIGHEST,
        preferred_element_type=F32,
    )
    part[...] = jnp.zeros_like(part)
    part[:, 0:dims] = gathered
    terms_ref[...] = terms
    sums_ref[...] = weight

    stores = [
        pltpu.make_async_copy(terms_ref, terms_hbm, local.at[0]),
        pltpu.make_async_copy(sums_ref, sums_hbm, local.at[1]),
    ]
    for copy in stores:
        copy.start()

    @pl.loop(1, n_all)
    def _(step):
        g_copy(step).start()

    @pl.loop(1, n)
    def _(slot):
        line_copy(slot).wait_send()

    @pl.loop(0, n)
    def _(slot):
        forward(slot).wait_send()

    for copy in stores:
        copy.wait()
    parts[0] = part[0:1]

    @pl.loop(1, n_all)
    def _(step):
        g_copy(step).wait()

    grad_ref[...] = (jnp.sum(parts[...], 0) / (row_count * n_all))[:, 0:dims]
    copy = pltpu.make_async_copy(grad_ref, grad_hbm, local.at[2])
    copy.start()
    copy.wait()


def on_device(row_size, col_size, x_rows, alpha_rows, x_cols, alpha_cols, lengthscale):
    dims, row_count = x_rows.shape
    col_count = x_cols.shape[1]
    n = row_size // CORES * col_size
    n_all = row_size * col_size
    anywhere = pl.BlockSpec(memory_space=pl.ANY)
    dma = pltpu.SemaphoreType.DMA
    terms, sums, grad = pl.pallas_call(
        functools.partial(kernel, row_size, col_size),
        out_shape=(
            jax.ShapeDtypeStruct((dims, row_count), F32),
            jax.ShapeDtypeStruct((1, row_count), F32),
            jax.ShapeDtypeStruct((1, dims), F32),
        ),
        in_specs=[anywhere] * 5,
        out_specs=(anywhere, anywhere, anywhere),
        scratch_shapes=[
            pltpu.VMEM((dims, row_count), F32),
            pltpu.VMEM((1, row_count), F32),
            pltpu.VMEM((1, dims), F32),
            pltpu.VMEM((dims, row_count), F32),
            pltpu.VMEM((1, row_count), F32),
            pltpu.VMEM((1, dims), F32),
            pltpu.VMEM((2 * n, dims + 1, col_count), F32),
            pltpu.VMEM((112, row_count), F32),
            pltpu.VMEM((112, row_count), BF16),
            pltpu.VMEM((8, 128), F32),
            pltpu.VMEM((n_all, 1, 128), F32),
            dma((5,)),
        ]
        + [dma((n,))] * 4
        + [dma((n_all,))] * 2,
        compiler_params=pltpu.CompilerParams(collective_id=0, has_side_effects=True),
    )(
        x_rows,
        alpha_rows.reshape(1, row_count),
        x_cols,
        alpha_cols.reshape(1, col_count),
        lengthscale.reshape(1, dims),
    )
    return terms, sums.reshape(row_count), grad.reshape(dims)


def solution(mesh):
    return jax.shard_map(
        functools.partial(on_device, mesh.shape["row"], mesh.shape["col"]),
        mesh=mesh,
        in_specs=(
            P(None, ("row", "col")),
            P(("row", "col")),
            P(None, ("col", "row")),
            P(("col", "row")),
            P(),
        ),
        out_specs=(P(None, ("row", "col")), P(("row", "col")), P()),
        check_vma=False,
    )
```

```python
import functools

import jax
import jax.numpy as jnp
from jax import lax
from jax.experimental import pallas as pl
from jax.experimental.pallas import tpu as pltpu
from jax.sharding import PartitionSpec as P

LOG2E = 1.4426950408889634
CORES = 2
MESH = pl.DeviceIdType.MESH
F32 = jnp.float32
BF16 = jnp.bfloat16


def split3(value):
    high = value.astype(BF16)
    rest = value - high.astype(F32)
    mid = rest.astype(BF16)
    low = (rest - mid.astype(F32)).astype(BF16)
    return high, mid, low


def stack_rows(count, rows):
    index = lax.broadcasted_iota(jnp.int32, (16, count), 0)
    out = jnp.zeros((16, count), F32)
    for place, row in enumerate(rows):
        row = row.astype(F32) if hasattr(row, "astype") else row
        out = jnp.where(index == place, row, out)
    return out.astype(BF16)


def kernel(
    row_size,
    col_size,
    xr_hbm,
    ar_hbm,
    xc_hbm,
    ac_hbm,
    ls_hbm,
    terms_hbm,
    sums_hbm,
    grad_hbm,
    xr_ref,
    ar_ref,
    ls_ref,
    terms_ref,
    sums_ref,
    grad_ref,
    chunks,
    acc,
    row_aug,
    part,
    parts,
    local,
    send_c,
    recv_c,
    send_f,
    recv_f,
    send_g,
    recv_g,
):
    dims, row_count = xr_ref.shape
    col_count = chunks.shape[2]
    n_x = row_size // CORES
    n_y = n_x if col_size % n_x == 0 else 1
    n_z = col_size // n_y
    n_plane = n_x * n_y
    n = n_x * col_size
    n_all = row_size * col_size
    my_row = lax.axis_index("row")
    my_col = lax.axis_index("col")
    my_z = my_col // n_y
    my_y = my_col % n_y
    partner = (my_row + 1 - 2 * (my_row % CORES), my_col)

    def line_peer(j):
        return (my_row, (my_z + j) % n_z * n_y + my_y)

    def plane_peer(m):
        return (
            (my_row + CORES * (m % n_x)) % row_size,
            my_z * n_y + (my_y + m // n_x) % n_y,
        )

    def any_peer(step):
        d_row = step % row_size
        d_col = step // row_size
        return ((my_row + d_row) % row_size, (my_col + d_col) % col_size)

    def loads():
        return [
            pltpu.make_async_copy(xc_hbm, chunks.at[0, pl.ds(0, dims)], local.at[0]),
            pltpu.make_async_copy(ac_hbm, chunks.at[0, pl.ds(dims, 1)], local.at[1]),
            pltpu.make_async_copy(xr_hbm, xr_ref, local.at[2]),
            pltpu.make_async_copy(ar_hbm, ar_ref, local.at[3]),
            pltpu.make_async_copy(ls_hbm, ls_ref, local.at[4]),
        ]

    for copy in loads():
        copy.start()

    barrier = pltpu.get_barrier_semaphore()

    pl.semaphore_signal(barrier, inc=1, device_id=partner, device_id_type=MESH)

    @pl.loop(1, n_plane)
    def _(m):
        pl.semaphore_signal(barrier, inc=1, device_id=plane_peer(m), device_id_type=MESH)

    @pl.loop(1, n_z)
    def _(j):
        pl.semaphore_signal(barrier, inc=1, device_id=line_peer(j), device_id_type=MESH)

    def line_copy(j):
        return pltpu.make_async_remote_copy(
            chunks.at[0], chunks.at[j], send_c.at[j], recv_c.at[j], line_peer(j), MESH
        )

    def plane_copy(j, m):
        slot = m * n_z + j
        return pltpu.make_async_remote_copy(
            chunks.at[j], chunks.at[slot], send_c.at[slot], recv_c.at[slot], plane_peer(m), MESH
        )

    def forward(slot):
        return pltpu.make_async_remote_copy(
            chunks.at[slot], chunks.at[n + slot], send_f.at[slot], recv_f.at[slot], partner, MESH
        )

    def g_copy(step):
        return pltpu.make_async_remote_copy(
            part.at[pl.ds(0, 1)],
            parts.at[step],
            send_g.at[step],
            recv_g.at[step],
            any_peer(step),
            MESH,
        )

    for copy in loads():
        copy.wait()

    eye = lax.broadcasted_iota(jnp.int32, (dims, dims), 0) == lax.broadcasted_iota(
        jnp.int32, (dims, dims), 1
    )
    scale = jnp.sum(jnp.where(eye, jnp.broadcast_to(ls_ref[...], (dims, dims)), 0.0), 1, keepdims=True)
    inverse = 1.0 / scale
    row_scaled = xr_ref[...] * inverse
    row_norm = (-0.5 * LOG2E) * jnp.sum(row_scaled * row_scaled, 0, keepdims=True)
    rh, rm, rl = split3(row_scaled * LOG2E)
    row_aug[...] = jnp.concatenate(
        [rh, rh, rh, rm, rm, rl, stack_rows(row_count, (1.0, 1.0, 1.0) + split3(row_norm))], 0
    )

    def operands(x, alpha):
        scaled = x * inverse
        norm = (-0.5 * LOG2E) * jnp.sum(scaled * scaled, 0, keepdims=True)
        ch, cm, cl = split3(scaled)
        col_aug = jnp.concatenate(
            [ch, cm, cl, ch, cm, ch, stack_rows(col_count, split3(norm) + (1.0, 1.0, 1.0))], 0
        )
        first = alpha * scaled
        fh, fm, fl = split3(first)
        sh, sm, sl = split3(first * scaled)
        group = stack_rows(col_count, split3(alpha))
        zero = jnp.zeros_like(fl)
        left_high = jnp.concatenate([fh, sh, fm, sm, fl, sl, group], 0)
        left_mid = jnp.concatenate([fh, sh, fm, sm, zero, zero, group], 0)
        exponent = lax.dot_general(
            col_aug, row_aug[...], (((0,), (0,)), ((), ())), preferred_element_type=F32
        )
        value = jnp.exp2(exponent)
        high = value.astype(BF16)
        mid = (value - high.astype(F32)).astype(BF16)
        return [left_high, left_mid], [high, mid]

    def contribute(slots):
        left, right = [], []
        for slot in slots:
            more_left, more_right = operands(
                chunks[slot, 0:dims], chunks[slot, dims : dims + 1]
            )
            left += more_left
            right += more_right
        return jnp.dot(
            jnp.concatenate(left, 1), jnp.concatenate(right, 0), preferred_element_type=F32
        )

    def in_groups(slots):
        slots = list(slots)
        for at in range(0, len(slots), 4):
            acc[...] += contribute(slots[at : at + 4])

    width = 2 if (n - n_z) % 2 == 0 else 1
    acc[...] = contribute([0])

    pl.semaphore_wait(barrier, n_plane + n_z - 1)

    @pl.loop(1, n_z)
    def _(j):
        line_copy(j).start()

    @pl.loop(1, n_plane)
    def _(m):
        plane_copy(0, m).start()

    forward(0).start()

    @pl.loop(1, n_z)
    def _(j):
        line_copy(j).wait_recv()

        @pl.loop(1, n_plane)
        def _(m):
            plane_copy(j, m).start()

        forward(j).start()

    forward(0).wait_recv()
    lag = n_z - 1
    in_groups([n] + list(range(1, n_z)))

    @pl.loop(0, (n - n_z) // width)
    def _(group):
        slots = [n_z + group * width + k for k in range(width)]
        for slot in slots:
            line_copy(slot).wait_recv()
            forward(slot).start()
        for slot in slots:
            forward(slot - lag).wait_recv()
        acc[...] += contribute(slots + [n + slot - lag for slot in slots])

    @pl.loop(n - lag, n)
    def _(slot):
        forward(slot).wait_recv()

    in_groups(range(2 * n - lag, 2 * n))

    total = acc[...]
    first = total[0:16] + total[32:48] + total[64:80]
    second = total[16:32] + total[48:64] + total[80:96]
    weight = total[96:97] + total[97:98] + total[98:99]
    terms = (0.5 * ar_ref[...]) * (
        row_scaled * row_scaled * weight - 2.0 * row_scaled * first + second
    )
    folded = terms[:, 0:128]
    for at in range(128, row_count, 128):
        folded = folded + terms[:, at : at + 128]
    gathered = lax.dot_general(
        jnp.ones((8, 128), F32),
        folded,
        (((1,), (1,)), ((), ())),
        precision=lax.Precision.HIGHEST,
        preferred_element_type=F32,
    )
    part[...] = jnp.zeros_like(part)
    part[:, 0:dims] = gathered
    terms_ref[...] = terms
    sums_ref[...] = weight

    stores = [
        pltpu.make_async_copy(terms_ref, terms_hbm, local.at[0]),
        pltpu.make_async_copy(sums_ref, sums_hbm, local.at[1]),
    ]
    for copy in stores:
        copy.start()

    @pl.loop(1, n_all)
    def _(step):
        g_copy(step).start()

    @pl.loop(1, n)
    def _(slot):
        line_copy(slot).wait_send()

    @pl.loop(0, n)
    def _(slot):
        forward(slot).wait_send()

    for copy in stores:
        copy.wait()
    parts[0] = part[0:1]

    @pl.loop(1, n_all)
    def _(step):
        g_copy(step).wait()

    grad_ref[...] = (jnp.sum(parts[...], 0) / (row_count * n_all))[:, 0:dims]
    copy = pltpu.make_async_copy(grad_ref, grad_hbm, local.at[2])
    copy.start()
    copy.wait()


def on_device(row_size, col_size, x_rows, alpha_rows, x_cols, alpha_cols, lengthscale):
    dims, row_count = x_rows.shape
    col_count = x_cols.shape[1]
    n = row_size // CORES * col_size
    n_all = row_size * col_size
    anywhere = pl.BlockSpec(memory_space=pl.ANY)
    dma = pltpu.SemaphoreType.DMA
    terms, sums, grad = pl.pallas_call(
        functools.partial(kernel, row_size, col_size),
        out_shape=(
            jax.ShapeDtypeStruct((dims, row_count), F32),
            jax.ShapeDtypeStruct((1, row_count), F32),
            jax.ShapeDtypeStruct((1, dims), F32),
        ),
        in_specs=[anywhere] * 5,
        out_specs=(anywhere, anywhere, anywhere),
        scratch_shapes=[
            pltpu.VMEM((dims, row_count), F32),
            pltpu.VMEM((1, row_count), F32),
            pltpu.VMEM((1, dims), F32),
            pltpu.VMEM((dims, row_count), F32),
            pltpu.VMEM((1, row_count), F32),
            pltpu.VMEM((1, dims), F32),
            pltpu.VMEM((2 * n, dims + 1, col_count), F32),
            pltpu.VMEM((112, row_count), F32),
            pltpu.VMEM((112, row_count), BF16),
            pltpu.VMEM((8, 128), F32),
            pltpu.VMEM((n_all, 1, 128), F32),
            dma((5,)),
        ]
        + [dma((n,))] * 4
        + [dma((n_all,))] * 2,
        compiler_params=pltpu.CompilerParams(collective_id=0, has_side_effects=True),
    )(
        x_rows,
        alpha_rows.reshape(1, row_count),
        x_cols,
        alpha_cols.reshape(1, col_count),
        lengthscale.reshape(1, dims),
    )
    return terms, sums.reshape(row_count), grad.reshape(dims)


def solution(mesh):
    return jax.shard_map(
        functools.partial(on_device, mesh.shape["row"], mesh.shape["col"]),
        mesh=mesh,
        in_specs=(
            P(None, ("row", "col")),
            P(("row", "col")),
            P(None, ("col", "row")),
            P(("col", "row")),
            P(),
        ),
        out_specs=(P(None, ("row", "col")), P(("row", "col")), P()),
        check_vma=False,
    )
```

```python
import functools

import jax
import jax.numpy as jnp
from jax import lax
from jax.experimental import pallas as pl
from jax.experimental.pallas import tpu as pltpu
from jax.sharding import PartitionSpec as P

LOG2E = 1.4426950408889634
CORES = 2
MESH = pl.DeviceIdType.MESH
F32 = jnp.float32
BF16 = jnp.bfloat16


def split3(value):
    high = value.astype(BF16)
    rest = value - high.astype(F32)
    mid = rest.astype(BF16)
    low = (rest - mid.astype(F32)).astype(BF16)
    return high, mid, low


def stack_rows(count, rows):
    index = lax.broadcasted_iota(jnp.int32, (16, count), 0)
    out = jnp.zeros((16, count), F32)
    for place, row in enumerate(rows):
        row = row.astype(F32) if hasattr(row, "astype") else row
        out = jnp.where(index == place, row, out)
    return out.astype(BF16)


def kernel(
    row_size,
    col_size,
    xr_hbm,
    ar_hbm,
    xc_hbm,
    ac_hbm,
    ls_hbm,
    terms_hbm,
    sums_hbm,
    grad_hbm,
    xr_ref,
    ar_ref,
    ls_ref,
    terms_ref,
    sums_ref,
    grad_ref,
    chunks,
    acc,
    row_aug,
    part,
    parts,
    local,
    send_c,
    recv_c,
    send_f,
    recv_f,
    send_g,
    recv_g,
):
    dims, row_count = xr_ref.shape
    col_count = chunks.shape[2]
    n_x = row_size // CORES
    n_y = n_x if col_size % n_x == 0 else 1
    n_z = col_size // n_y
    n_plane = n_x * n_y
    n = n_x * col_size
    n_all = row_size * col_size
    my_row = lax.axis_index("row")
    my_col = lax.axis_index("col")
    my_z = my_col // n_y
    my_y = my_col % n_y
    partner = (my_row + 1 - 2 * (my_row % CORES), my_col)

    def line_peer(j):
        return (my_row, (my_z + j) % n_z * n_y + my_y)

    def plane_peer(m):
        return (
            (my_row + CORES * (m % n_x)) % row_size,
            my_z * n_y + (my_y + m // n_x) % n_y,
        )

    def any_peer(step):
        d_row = step % row_size
        d_col = step // row_size
        return ((my_row + d_row) % row_size, (my_col + d_col) % col_size)

    def loads():
        return [
            pltpu.make_async_copy(xc_hbm, chunks.at[0, pl.ds(0, dims)], local.at[0]),
            pltpu.make_async_copy(ac_hbm, chunks.at[0, pl.ds(dims, 1)], local.at[1]),
            pltpu.make_async_copy(xr_hbm, xr_ref, local.at[2]),
            pltpu.make_async_copy(ar_hbm, ar_ref, local.at[3]),
            pltpu.make_async_copy(ls_hbm, ls_ref, local.at[4]),
        ]

    for copy in loads():
        copy.start()

    barrier = pltpu.get_barrier_semaphore()

    pl.semaphore_signal(barrier, inc=1, device_id=partner, device_id_type=MESH)

    @pl.loop(1, n_plane)
    def _(m):
        pl.semaphore_signal(barrier, inc=1, device_id=plane_peer(m), device_id_type=MESH)

    @pl.loop(1, n_z)
    def _(j):
        pl.semaphore_signal(barrier, inc=1, device_id=line_peer(j), device_id_type=MESH)

    def line_copy(j):
        return pltpu.make_async_remote_copy(
            chunks.at[0], chunks.at[j], send_c.at[j], recv_c.at[j], line_peer(j), MESH
        )

    def plane_copy(j, m):
        slot = m * n_z + j
        return pltpu.make_async_remote_copy(
            chunks.at[j], chunks.at[slot], send_c.at[slot], recv_c.at[slot], plane_peer(m), MESH
        )

    def forward(slot):
        return pltpu.make_async_remote_copy(
            chunks.at[slot], chunks.at[n + slot], send_f.at[slot], recv_f.at[slot], partner, MESH
        )

    def g_copy(step):
        return pltpu.make_async_remote_copy(
            part.at[pl.ds(0, 1)],
            parts.at[step],
            send_g.at[step],
            recv_g.at[step],
            any_peer(step),
            MESH,
        )

    for copy in loads():
        copy.wait()

    eye = lax.broadcasted_iota(jnp.int32, (dims, dims), 0) == lax.broadcasted_iota(
        jnp.int32, (dims, dims), 1
    )
    scale = jnp.sum(jnp.where(eye, jnp.broadcast_to(ls_ref[...], (dims, dims)), 0.0), 1, keepdims=True)
    inverse = 1.0 / scale
    row_scaled = xr_ref[...] * inverse
    row_norm = (-0.5 * LOG2E) * jnp.sum(row_scaled * row_scaled, 0, keepdims=True)
    rh, rm, rl = split3(row_scaled * LOG2E)
    row_aug[...] = jnp.concatenate(
        [rh, rh, rh, rm, rm, rl, stack_rows(row_count, (1.0, 1.0, 1.0) + split3(row_norm))], 0
    )

    def operands(x, alpha):
        scaled = x * inverse
        norm = (-0.5 * LOG2E) * jnp.sum(scaled * scaled, 0, keepdims=True)
        ch, cm, cl = split3(scaled)
        col_aug = jnp.concatenate(
            [ch, cm, cl, ch, cm, ch, stack_rows(col_count, split3(norm) + (1.0, 1.0, 1.0))], 0
        )
        first = alpha * scaled
        fh, fm, fl = split3(first)
        sh, sm, sl = split3(first * scaled)
        group = stack_rows(col_count, split3(alpha))
        zero = jnp.zeros_like(fl)
        left_high = jnp.concatenate([fh, sh, fm, sm, fl, sl, group], 0)
        left_mid = jnp.concatenate([fh, sh, fm, sm, zero, zero, group], 0)
        exponent = lax.dot_general(
            col_aug, row_aug[...], (((0,), (0,)), ((), ())), preferred_element_type=F32
        )
        value = jnp.exp2(exponent)
        high = value.astype(BF16)
        mid = (value - high.astype(F32)).astype(BF16)
        return [left_high, left_mid], [high, mid]

    def contribute(slots):
        left, right = [], []
        for slot in slots:
            more_left, more_right = operands(
                chunks[slot, 0:dims], chunks[slot, dims : dims + 1]
            )
            left += more_left
            right += more_right
        return jnp.dot(
            jnp.concatenate(left, 1), jnp.concatenate(right, 0), preferred_element_type=F32
        )

    def in_groups(slots):
        slots = list(slots)
        for at in range(0, len(slots), 4):
            acc[...] += contribute(slots[at : at + 4])

    width = 2 if (n - n_z) % 2 == 0 else 1
    acc[...] = contribute([0])

    pl.semaphore_wait(barrier, n_plane + n_z - 1)

    @pl.loop(1, n_z)
    def _(j):
        line_copy(j).start()

    @pl.loop(1, n_plane)
    def _(m):
        plane_copy(0, m).start()

    forward(0).start()

    @pl.loop(1, n_z)
    def _(j):
        line_copy(j).wait_recv()

        @pl.loop(1, n_plane)
        def _(m):
            plane_copy(j, m).start()

        forward(j).start()

    forward(0).wait_recv()
    lag = n_z - 1
    in_groups([n] + list(range(1, n_z)))

    @pl.loop(0, (n - n_z) // width)
    def _(group):
        slots = [n_z + group * width + k for k in range(width)]
        for slot in slots:
            line_copy(slot).wait_recv()
            forward(slot).start()
        for slot in slots:
            forward(slot - lag).wait_recv()
        acc[...] += contribute(slots + [n + slot - lag for slot in slots])

    @pl.loop(n - lag, n)
    def _(slot):
        forward(slot).wait_recv()

    in_groups(range(2 * n - lag, 2 * n))

    total = acc[...]
    first = total[0:16] + total[32:48] + total[64:80]
    second = total[16:32] + total[48:64] + total[80:96]
    weight = total[96:97] + total[97:98] + total[98:99]
    terms = (0.5 * ar_ref[...]) * (
        row_scaled * row_scaled * weight - 2.0 * row_scaled * first + second
    )
    folded = terms[:, 0:128]
    for at in range(128, row_count, 128):
        folded = folded + terms[:, at : at + 128]
    gathered = lax.dot_general(
        jnp.ones((8, 128), F32),
        folded,
        (((1,), (1,)), ((), ())),
        precision=lax.Precision.HIGHEST,
        preferred_element_type=F32,
    )
    part[...] = jnp.zeros_like(part)
    part[:, 0:dims] = gathered
    terms_ref[...] = terms
    sums_ref[...] = weight

    stores = [
        pltpu.make_async_copy(terms_ref, terms_hbm, local.at[0]),
        pltpu.make_async_copy(sums_ref, sums_hbm, local.at[1]),
    ]
    for copy in stores:
        copy.start()

    @pl.loop(1, n_all)
    def _(step):
        g_copy(step).start()

    @pl.loop(1, n)
    def _(slot):
        line_copy(slot).wait_send()

    @pl.loop(0, n)
    def _(slot):
        forward(slot).wait_send()

    for copy in stores:
        copy.wait()
    parts[0] = part[0:1]

    @pl.loop(1, n_all)
    def _(step):
        g_copy(step).wait()

    grad_ref[...] = (jnp.sum(parts[...], 0) / (row_count * n_all))[:, 0:dims]
    copy = pltpu.make_async_copy(grad_ref, grad_hbm, local.at[2])
    copy.start()
    copy.wait()


def settle(terms_in, sums_in, grad_in, terms_out, sums_out, grad_out):
    terms_out[...] = terms_in[...]
    sums_out[...] = sums_in[...]
    grad_out[...] = grad_in[...]


def on_device(row_size, col_size, x_rows, alpha_rows, x_cols, alpha_cols, lengthscale):
    dims, row_count = x_rows.shape
    col_count = x_cols.shape[1]
    n = row_size // CORES * col_size
    n_all = row_size * col_size
    vmem = pl.BlockSpec(memory_space=pltpu.VMEM)
    anywhere = pl.BlockSpec(memory_space=pl.ANY)
    dma = pltpu.SemaphoreType.DMA
    terms, sums, grad = pl.pallas_call(
        functools.partial(kernel, row_size, col_size),
        out_shape=(
            jax.ShapeDtypeStruct((dims, row_count), F32),
            jax.ShapeDtypeStruct((1, row_count), F32),
            jax.ShapeDtypeStruct((1, dims), F32),
        ),
        in_specs=[anywhere] * 5,
        out_specs=(anywhere, anywhere, anywhere),
        scratch_shapes=[
            pltpu.VMEM((dims, row_count), F32),
            pltpu.VMEM((1, row_count), F32),
            pltpu.VMEM((1, dims), F32),
            pltpu.VMEM((dims, row_count), F32),
            pltpu.VMEM((1, row_count), F32),
            pltpu.VMEM((1, dims), F32),
            pltpu.VMEM((2 * n, dims + 1, col_count), F32),
            pltpu.VMEM((112, row_count), F32),
            pltpu.VMEM((112, row_count), BF16),
            pltpu.VMEM((8, 128), F32),
            pltpu.VMEM((n_all, 1, 128), F32),
            dma((5,)),
        ]
        + [dma((n,))] * 4
        + [dma((n_all,))] * 2,
        compiler_params=pltpu.CompilerParams(collective_id=0, has_side_effects=True),
    )(
        x_rows,
        alpha_rows.reshape(1, row_count),
        x_cols,
        alpha_cols.reshape(1, col_count),
        lengthscale.reshape(1, dims),
    )
    terms, sums, grad = pl.pallas_call(
        settle,
        out_shape=(terms, sums, grad),
        in_specs=[vmem] * 3,
        out_specs=(vmem, vmem, vmem),
    )(terms, sums, grad)
    return terms, sums.reshape(row_count), grad.reshape(dims)


def solution(mesh):
    return jax.shard_map(
        functools.partial(on_device, mesh.shape["row"], mesh.shape["col"]),
        mesh=mesh,
        in_specs=(
            P(None, ("row", "col")),
            P(("row", "col")),
            P(None, ("col", "row")),
            P(("col", "row")),
            P(),
        ),
        out_specs=(P(None, ("row", "col")), P(("row", "col")), P()),
        check_vma=False,
    )
```
